64 devices in a mesh: rep: 8 (over x, y, core), dp: 8 (over z).
Axes of the slice: x: 2, y: 2, z: 8, core: 2. Of those that a mesh axis runs over, the one named last changes fastest.
The devices are a block of a 4x4x8 slice.
Arguments:
- a: bfloat16 [64, 4, 4096, 768], P(('rep', 'dp')), parts along dimension 0
- g: bfloat16 [64, 4, 4096, 3072], P(('rep', 'dp')), parts along dimension 0
Outputs:
- output: bfloat16 [32, 768, 3072], P('rep'), parts along dimension 0
There are 8 independent parts. The reference program is written for one: setup_inputs(seed, part) draws one part's arguments, and reference() takes and returns one part's arrays. A program takes and returns all parts, laid end to end along the dimension named above; each array names one.
All inputs are finite; a program needn't handle non-finite values.
Results may differ from the reference program's by a relative error of at most 0.012.
Values are sent between devices in bfloat16 or wider.
A program may use at most 768 MiB of HBM per device.

```python
import jax
import jax.numpy as jnp
from jax import lax

DEVICES = 8
MATRICES = 4
TOKENS = 4096
D = 768
FF = 3072


def setup_inputs(seed: int = 0, part: int = 0) -> dict:
    ka, kg, ks = (jax.random.fold_in(k, part) for k in jax.random.split(jax.random.key(seed), 3))
    size = 2.0 ** jax.random.uniform(ks, (DEVICES, MATRICES, 1, 1), jnp.float32, -1.0, 1.0)
    a = jax.random.normal(ka, (DEVICES, MATRICES, TOKENS, D), jnp.float32)
    g = size * jax.random.normal(kg, (DEVICES, MATRICES, TOKENS, FF), jnp.float32) * (DEVICES * TOKENS) ** -0.5
    return {"a": a.astype(jnp.bfloat16), "g": g.astype(jnp.bfloat16)}


def reference(a, g):
    def take(so_far, one):
        return so_far + jnp.einsum("ntd,ntf->ndf", *one, preferred_element_type=jnp.float32), None

    return lax.scan(take, jnp.zeros((MATRICES, D, FF), jnp.float32), (a, g))[0].astype(jnp.bfloat16)
```

```python
import functools

import jax
import jax.numpy as jnp
from jax import lax
from jax.experimental import pallas as pl
from jax.experimental.pallas import tpu as pltpu
from jax.sharding import PartitionSpec as P

MESH = pl.DeviceIdType.MESH
STREAMS = 2
PIECES = 4


def ring_kernel(
    size, a_hbm, g_hbm, sums, a_vmem, g_vmem, term, a_sem, g_sem, send_sem, recv_sem
):
    matrices, tokens, rows = a_hbm.shape
    columns = g_hbm.shape[2]
    half, width, piece = rows // 2, columns // size, tokens // PIECES
    rounds = matrices // STREAMS
    hops = 2 * (size - 1)
    per_round = hops * STREAMS
    halfsteps = rounds * per_round
    items = rounds * size * STREAMS

    me = lax.axis_index("dp")
    right, left = lax.rem(me + 1, size), lax.rem(me + size - 1, size)

    def place(h):
        r = lax.rem(h, per_round)
        x = lax.rem(r, STREAMS)
        return (h // per_round) * STREAMS + x, r // STREAMS, x

    def chunk(k, way):
        return lax.rem(me + 2 * size + (k if way else -k), size)

    def a_copy(n, x, j):
        part = pl.ds(pl.multiple_of(j * piece, piece), piece)
        return pltpu.make_async_copy(
            a_hbm.at[n, part, :], a_vmem.at[x, part, :], a_sem.at[x, j]
        )

    def g_copy(i, way, j):
        q, r = i // (size * STREAMS), lax.rem(i, size * STREAMS)
        n, k = q * STREAMS + lax.rem(r, STREAMS), r // STREAMS
        part = pl.ds(pl.multiple_of(j * piece, piece), piece)
        block = pl.ds(pl.multiple_of(chunk(k, way) * width, width), width)
        slot = lax.rem(i, 2)
        return pltpu.make_async_copy(
            g_hbm.at[n, part, block],
            g_vmem.at[slot, way, part, :],
            g_sem.at[slot, way, j],
        )

    def start_g(i):
        for j in range(PIECES):
            for way in range(2):
                g_copy(i, way, j).start()

    def view(n, k, way):
        block = pl.ds(pl.multiple_of(chunk(k, way) * width, width), width)
        return sums.at[n, pl.ds(way * half, half), block]

    def remote(h, way):
        n, k, _ = place(h)
        ref = view(n, k, way)
        return pltpu.make_async_remote_copy(
            src_ref=ref,
            dst_ref=ref,
            send_sem=send_sem.at[h, way],
            recv_sem=recv_sem.at[h, way],
            device_id={"dp": left if way else right},
            device_id_type=MESH,
        )

    for j in range(PIECES):
        a_copy(0, 0, j).start()
        for way in range(2):
            g_copy(0, way, j).start()

    barrier = pltpu.get_barrier_semaphore()
    for neighbour in (left, right):
        pl.semaphore_signal(
            barrier, inc=1, device_id={"dp": neighbour}, device_id_type=MESH
        )
    pl.semaphore_wait(barrier, 2)

    def communicate(h):
        n, k, _ = place(h)

        @pl.when(h >= STREAMS)
        def _():
            for way in range(2):
                remote(h - STREAMS, way).wait_recv()
            for way in range(2):
                remote(h - STREAMS, way).wait_send()

        @pl.when(k == 0)
        def _():
            for way in range(2):
                view(n, k, way)[...] = term[way].astype(sums.dtype)

        @pl.when((k > 0) & (k < size))
        def _():
            for way in range(2):
                ref = view(n, k, way)
                ref[...] = (ref[...].astype(jnp.float32) + term[way]).astype(sums.dtype)

        for way in range(2):
            remote(h, way).start()

    def compute(h):
        n, k, x = place(h)
        q = n // STREAMS
        i = q * size * STREAMS + k * STREAMS + x
        slot = lax.rem(i, 2)
        term[...] = jnp.zeros_like(term)

        @pl.loop(0, PIECES)
        def _(j):
            @pl.when(k == 0)
            def _():
                a_copy(n, x, j).wait()

            for way in range(2):
                g_copy(i, way, j).wait()

            @pl.when((j == 2) & (i + 1 < items))
            def _():
                start_g(i + 1)

            @pl.when((j == 2) & (i == 0))
            def _():
                for x1 in range(1, STREAMS):
                    for j1 in range(PIECES):
                        a_copy(x1, x1, j1).start()

            part = pl.ds(pl.multiple_of(j * piece, piece), piece)
            for way in range(2):
                term[way] += lax.dot_general(
                    a_vmem[x, part, way * half : (way + 1) * half],
                    g_vmem[slot, way, part, :],
                    (((0,), (0,)), ((), ())),
                    preferred_element_type=jnp.float32,
                )

        @pl.when((k == size - 1) & (q < rounds - 1))
        def _():
            for j in range(PIECES):
                a_copy(n + STREAMS, x, j).start()

    @pl.loop(0, halfsteps + 1)
    def _(t):
        @pl.when(t > 0)
        def _():
            communicate(t - 1)

        @pl.when((t < halfsteps) & (lax.rem(t, per_round) // STREAMS < size))
        def _():
            compute(t)

    for h in range(halfsteps - STREAMS, halfsteps):
        for way in range(2):
            remote(h, way).wait_recv()
        for way in range(2):
            remote(h, way).wait_send()


def solution(mesh):
    size = mesh.shape["dp"]

    def step(a, g):
        a, g = a[0], g[0]
        matrices, tokens, rows = a.shape
        columns = g.shape[2]
        half, width = rows // 2, columns // size
        halfsteps = matrices * 2 * (size - 1)
        shape = (matrices, rows, columns)
        return pl.pallas_call(
            functools.partial(ring_kernel, size),
            out_shape=pltpu.VMEM(shape, jnp.bfloat16),
            in_specs=[pl.BlockSpec(memory_space=pltpu.HBM)] * 2,
            out_specs=pl.BlockSpec(memory_space=pltpu.VMEM),
            scratch_shapes=[
                pltpu.VMEM((STREAMS, tokens, rows), jnp.bfloat16),
                pltpu.VMEM((2, 2, tokens, width), jnp.bfloat16),
                pltpu.VMEM((2, half, width), jnp.float32),
                pltpu.SemaphoreType.DMA((STREAMS, PIECES)),
                pltpu.SemaphoreType.DMA((2, 2, PIECES)),
                pltpu.SemaphoreType.DMA((halfsteps, 2)),
                pltpu.SemaphoreType.DMA((halfsteps, 2)),
            ],
            compiler_params=pltpu.CompilerParams(
                collective_id=0,
                has_side_effects=True,
                vmem_limit_bytes=36 * 1024 * 1024,
            ),
            cost_estimate=pl.CostEstimate(
                flops=2 * matrices * tokens * rows * columns,
                bytes_accessed=2 * matrices * tokens * (rows + 2 * columns),
                transcendentals=0,
            ),
        )(a, g)

    return jax.shard_map(
        step,
        mesh=mesh,
        in_specs=(P(("rep", "dp")), P(("rep", "dp"))),
        out_specs=P("rep"),
        check_vma=False,
    )
```

```python
import functools

import jax
import jax.numpy as jnp
from jax import lax
from jax.experimental import pallas as pl
from jax.experimental.pallas import tpu as pltpu
from jax.sharding import PartitionSpec as P

MESH = pl.DeviceIdType.MESH
STREAMS = 2
JOINED = 2
PIECES = 4
STRIP = 128


def ring_kernel(
    size, a_hbm, g_hbm, sums, a_vmem, g_vmem, term, a_sem, g_sem, send_sem, recv_sem
):
    matrices, tokens, rows = a_hbm.shape
    columns = g_hbm.shape[2]
    strips, width, piece = rows // (2 * STRIP), columns // size, tokens // PIECES
    rounds = matrices // STREAMS
    per_round = 2 * (size - 1) * STREAMS
    halfsteps = rounds * per_round
    items = rounds * size * STREAMS
    parts = [(s, 0, width) for s in range(strips)]

    me = lax.axis_index("dp")
    right, left = lax.rem(me + 1, size), lax.rem(me + size - 1, size)

    def place(h):
        r = lax.rem(h, per_round)
        x = lax.rem(r, STREAMS)
        return (h // per_round) * STREAMS + x, r // STREAMS, x

    def block(k, way, first=0, last=width):
        c = lax.rem(me + 2 * size + (k if way else -k), size)
        return pl.ds(pl.multiple_of(c * width + first, STRIP), last - first)

    def tokens_of(j):
        return pl.ds(pl.multiple_of(j * piece, piece), piece)

    def a_copy(n, x, j):
        return pltpu.make_async_copy(
            a_hbm.at[n, tokens_of(j), :], a_vmem.at[x, tokens_of(j), :], a_sem.at[x, j]
        )

    def first_a_copy(s, j):
        strip = pl.ds(2 * STRIP * s, 2 * STRIP)
        return pltpu.make_async_copy(
            a_hbm.at[0, tokens_of(j), strip],
            a_vmem.at[0, tokens_of(j), strip],
            a_sem.at[s + STREAMS - 1 if s else 0, j],
        )

    def first_g_copy(p, j):
        _, first, last = parts[p]
        return pltpu.make_async_copy(
            g_hbm.at[0, tokens_of(j), block(0, 0, first, last)],
            g_vmem.at[0, 0, tokens_of(j), pl.ds(first, last - first)],
            g_sem.at[0, 0, j],
        )

    def item_place(i):
        q, r = i // (size * STREAMS), lax.rem(i, size * STREAMS)
        return q * STREAMS + lax.rem(r, STREAMS), r // STREAMS

    def g_copy(i, way, j):
        n, k = item_place(i)
        slot = lax.rem(i, 2)
        return pltpu.make_async_copy(
            g_hbm.at[n, tokens_of(j), block(k, way)],
            g_vmem.at[slot, way, tokens_of(j), :],
            g_sem.at[slot, way, j],
        )

    def apart(k):
        return (lax.rem(k, size // 2) + size // 2 - 1) // (size // 2)

    def start_g(i):
        _, k = item_place(i)
        for j in range(PIECES):
            g_copy(i, 0, j).start()

            @pl.when(apart(k) == 1)
            def _():
                g_copy(i, 1, j).start()

    def remote(h, way):
        n, k, _ = place(h)
        ref = sums.at[n, :, way, :, block(k, way)]
        sem = lax.rem(h, 2 * STREAMS)
        return pltpu.make_async_remote_copy(
            src_ref=ref,
            dst_ref=ref,
            send_sem=send_sem.at[sem, way],
            recv_sem=recv_sem.at[sem, way],
            device_id={"dp": left if way else right},
            device_id_type=MESH,
        )

    def remote_part(p, way):
        s, first, last = parts[p]
        ref = sums.at[0, s, way, :, block(0, way, first, last)]
        sem = 2 * STREAMS + p
        return pltpu.make_async_remote_copy(
            src_ref=ref,
            dst_ref=ref,
            send_sem=send_sem.at[sem, way],
            recv_sem=recv_sem.at[sem, way],
            device_id={"dp": left if way else right},
            device_id_type=MESH,
        )

    def matmul(lhs, rhs):
        return lax.dot_general(
            lhs, rhs, (((0,), (0,)), ((), ())), preferred_element_type=jnp.float32
        )

    def compute_part(s):
        strip = slice(2 * STRIP * s, 2 * STRIP * (s + 1))
        if s == 0:
            term[:, 0] = jnp.zeros((2, STRIP, width), jnp.float32)

            @pl.loop(0, PIECES)
            def _(j):
                first_a_copy(0, j).wait()
                first_g_copy(0, j).wait()

                @pl.when(j == 1)
                def _():
                    for s1 in range(1, strips):
                        for j1 in range(PIECES):
                            first_a_copy(s1, j1).start()

                @pl.when(j == PIECES - 1)
                def _():
                    for j1 in range(PIECES):
                        for x in range(1, STREAMS):
                            a_copy(x, x, j1).start()
                        g_copy(1, 0, j1).start()

                product = matmul(
                    a_vmem[0, tokens_of(j), strip], g_vmem[0, 0, tokens_of(j), :]
                )
                term[:, 0] += product.reshape(2, STRIP, width)

        else:
            for j in range(PIECES):
                first_a_copy(s, j).wait()
            product = matmul(a_vmem[0, :, strip], g_vmem[0, 0])
            term[:, s] = product.reshape(2, STRIP, width)
        for way in range(2):
            sums[0, s, way, :, block(0, way)] = term[way, s].astype(sums.dtype)

    def communicate(h):
        n, k, _ = place(h)

        @pl.when(h == STREAMS)
        def _():
            for p in range(len(parts)):
                for way in range(2):
                    remote_part(p, way).wait()

        @pl.when(h > STREAMS)
        def _():
            for way in range(2):
                remote(h - STREAMS, way).wait()

        @pl.when(k == 0)
        def _():
            for way in range(2):
                sums[n, :, way, :, block(k, way)] = term[way].astype(sums.dtype)

        @pl.when((k > 0) & (k < size))
        def _():
            for way in range(2):
                cols = block(k, way)
                came = sums[n, :, way, :, cols].astype(jnp.float32)
                sums[n, :, way, :, cols] = (came + term[way]).astype(sums.dtype)

        for way in range(2):
            remote(h, way).start()

    def compute(h):
        n, k, x = place(h)
        q = n // STREAMS
        i = q * size * STREAMS + k * STREAMS + x
        slot = lax.rem(i, 2)
        term[...] = jnp.zeros_like(term)

        @pl.loop(0, PIECES // JOINED)
        def _(jj):
            for j in range(JOINED):
                load = jj * JOINED + j

                @pl.when(k == 0)
                def _():
                    a_copy(n, x, load).wait()

                g_copy(i, 0, load).wait()

                @pl.when(apart(k) == 1)
                def _():
                    g_copy(i, 1, load).wait()

            @pl.when((jj == 0) & (i + 1 < items))
            def _():
                start_g(i + 1)

            part = pl.ds(pl.multiple_of(jj * JOINED * piece, piece), JOINED * piece)
            lhs = a_vmem[x, part, :]
            for way in range(2):
                strip = [
                    lhs[:, (2 * s + way) * STRIP : (2 * s + way + 1) * STRIP]
                    for s in range(strips)
                ]
                product = matmul(
                    jnp.concatenate(strip, axis=1),
                    g_vmem[slot, way * apart(k), part, :],
                )
                term[way] += product.reshape(strips, STRIP, width)

        @pl.when((k == size - 1) & (q < rounds - 1))
        def _():
            for j in range(PIECES):
                a_copy(n + STREAMS, x, j).start()

    barrier = pltpu.get_barrier_semaphore()
    for neighbour in (left, right):
        pl.semaphore_signal(
            barrier, inc=1, device_id={"dp": neighbour}, device_id_type=MESH
        )
    for j in range(PIECES):
        first_a_copy(0, j).start()
        first_g_copy(0, j).start()
    for p in range(len(parts)):
        compute_part(p)
        if p == 0:
            pl.semaphore_wait(barrier, 2)
        for way in range(2):
            remote_part(p, way).start()

    @pl.loop(1, halfsteps + 1)
    def _(t):
        @pl.when(t > 1)
        def _():
            communicate(t - 1)

        @pl.when((t < halfsteps) & (lax.rem(t, per_round) // STREAMS < size))
        def _():
            compute(t)

    for h in range(halfsteps - STREAMS, halfsteps):
        for way in range(2):
            remote(h, way).wait()


def store_kernel(sums, out, sem):
    copies = [
        pltpu.make_async_copy(sums.at[n], out.at[n], sem.at[n])
        for n in range(sums.shape[0])
    ]
    for copy in copies:
        copy.start()
    for copy in copies:
        copy.wait()


def solution(mesh):
    size = mesh.shape["dp"]

    def step(a, g):
        a, g = a[0], g[0]
        matrices, tokens, rows = a.shape
        columns = g.shape[2]
        strips, width = rows // (2 * STRIP), columns // size
        parts = strips
        shape = (matrices, strips, 2, STRIP, columns)
        sums = pl.pallas_call(
            functools.partial(ring_kernel, size),
            out_shape=pltpu.VMEM(shape, jnp.bfloat16),
            in_specs=[pl.BlockSpec(memory_space=pltpu.HBM)] * 2,
            out_specs=pl.BlockSpec(memory_space=pltpu.VMEM),
            scratch_shapes=[
                pltpu.VMEM((STREAMS, tokens, rows), jnp.bfloat16),
                pltpu.VMEM((2, 2, tokens, width), jnp.bfloat16),
                pltpu.VMEM((2, strips, STRIP, width), jnp.float32),
                pltpu.SemaphoreType.DMA((STREAMS + strips - 1, PIECES)),
                pltpu.SemaphoreType.DMA((2, 2, PIECES)),
                pltpu.SemaphoreType.DMA((2 * STREAMS + parts, 2)),
                pltpu.SemaphoreType.DMA((2 * STREAMS + parts, 2)),
            ],
            compiler_params=pltpu.CompilerParams(
                collective_id=0,
                has_side_effects=True,
                vmem_limit_bytes=36 * 1024 * 1024,
            ),
            cost_estimate=pl.CostEstimate(
                flops=2 * matrices * tokens * rows * columns,
                bytes_accessed=2 * matrices * tokens * (rows + 2 * columns),
                transcendentals=0,
            ),
        )(a, g)
        out = pl.pallas_call(
            store_kernel,
            out_shape=jax.ShapeDtypeStruct(shape, jnp.bfloat16),
            in_specs=[pl.BlockSpec(memory_space=pltpu.VMEM)],
            out_specs=pl.BlockSpec(memory_space=pltpu.HBM),
            scratch_shapes=[pltpu.SemaphoreType.DMA((matrices,))],
            compiler_params=pltpu.CompilerParams(vmem_limit_bytes=20 * 1024 * 1024),
        )(sums)
        return out.reshape(matrices, rows, columns)

    return jax.shard_map(
        step,
        mesh=mesh,
        in_specs=(P(("rep", "dp")), P(("rep", "dp"))),
        out_specs=P("rep"),
        check_vma=False,
    )
```

```python
import functools

import jax
import jax.numpy as jnp
from jax import lax
from jax.experimental import pallas as pl
from jax.experimental.pallas import tpu as pltpu
from jax.sharding import PartitionSpec as P

MESH = pl.DeviceIdType.MESH
STREAMS = 2
HALVES = 2
PIECES = 4
STRIP = 128


def ring_kernel(
    size,
    a_hbm,
    g_hbm,
    sums,
    a_vmem,
    g_vmem,
    term,
    first_sem,
    strip_sem,
    a_sem,
    g_sem,
    send_sem,
    recv_sem,
):
    matrices, tokens, rows = a_hbm.shape
    columns = g_hbm.shape[2]
    strips, width = rows // (2 * STRIP), columns // size
    rounds = matrices // STREAMS
    per_round = 2 * (size - 1) * STREAMS
    halfsteps = rounds * per_round
    items = rounds * size * STREAMS
    me = lax.axis_index("dp")
    right, left = lax.rem(me + 1, size), lax.rem(me + size - 1, size)

    def place(h):
        r = lax.rem(h, per_round)
        x = lax.rem(r, STREAMS)
        return (h // per_round) * STREAMS + x, r // STREAMS, x

    def block(k, way, first=0, last=width):
        c = lax.rem(me + 2 * size + (k if way else -k), size)
        return pl.ds(pl.multiple_of(c * width + first, STRIP), last - first)

    def tokens_of(j, count):
        part = tokens // count
        return pl.ds(pl.multiple_of(j * part, part), part)

    def a_copy(n, x, j):
        part = tokens_of(j, HALVES)
        return pltpu.make_async_copy(
            a_hbm.at[n, part, :], a_vmem.at[x, part, :], a_sem.at[x, j]
        )

    def strip_of(s):
        return pl.ds(pl.multiple_of(2 * STRIP * s, 2 * STRIP), 2 * STRIP)

    def first_copies(j):
        part = tokens_of(j, PIECES)
        return (
            pltpu.make_async_copy(
                a_hbm.at[0, part, strip_of(0)],
                a_vmem.at[0, part, strip_of(0)],
                first_sem.at[0, j],
            ),
            pltpu.make_async_copy(
                g_hbm.at[0, part, block(0, 0, 0, STRIP)],
                g_vmem.at[0, 0, part, pl.ds(0, STRIP)],
                first_sem.at[1, j],
            ),
        )

    def first_g_copy():
        return pltpu.make_async_copy(
            g_hbm.at[0, :, block(0, 0, STRIP, width)],
            g_vmem.at[0, 0, :, pl.ds(STRIP, width - STRIP)],
            g_sem.at[0, 0, 0],
        )

    def first_a_copy(s):
        return pltpu.make_async_copy(
            a_hbm.at[0, :, strip_of(s)], a_vmem.at[0, :, strip_of(s)], strip_sem.at[s]
        )

    def item_place(i):
        q, r = i // (size * STREAMS), lax.rem(i, size * STREAMS)
        return q * STREAMS + lax.rem(r, STREAMS), r // STREAMS

    def g_copy(i, way, j):
        n, k = item_place(i)
        slot = lax.rem(i, 2)
        return pltpu.make_async_copy(
            g_hbm.at[n, tokens_of(j, HALVES), block(k, way)],
            g_vmem.at[slot, way, tokens_of(j, HALVES), :],
            g_sem.at[slot, way, j],
        )

    def apart(k):
        return (lax.rem(k, size // 2) + size // 2 - 1) // (size // 2)

    def start_g(i):
        _, k = item_place(i)
        for j in range(HALVES):
            g_copy(i, 0, j).start()

            @pl.when(apart(k) == 1)
            def _():
                g_copy(i, 1, j).start()

    def remote(h, way):
        n, k, _ = place(h)
        ref = sums.at[n, :, way, :, block(k, way)]
        sem = lax.rem(h, 2 * STREAMS)
        return pltpu.make_async_remote_copy(
            src_ref=ref,
            dst_ref=ref,
            send_sem=send_sem.at[sem, way],
            recv_sem=recv_sem.at[sem, way],
            device_id={"dp": left if way else right},
            device_id_type=MESH,
        )

    def remote_part(r, way, first=0, last=width):
        x, s = r // strips, lax.rem(r, strips)
        ref = sums.at[x, s, way, :, block(0, way, first, last)]
        return pltpu.make_async_remote_copy(
            src_ref=ref,
            dst_ref=ref,
            send_sem=send_sem.at[x, way],
            recv_sem=recv_sem.at[x, way],
            device_id={"dp": left if way else right},
            device_id_type=MESH,
        )

    def matmul(lhs, rhs):
        return lax.dot_general(
            lhs, rhs, (((0,), (0,)), ((), ())), preferred_element_type=jnp.float32
        )

    def send_part(r, first=0, last=width):
        x, s = r // strips, lax.rem(r, strips)
        for way in range(2):
            sums[x, s, way, :, block(0, way, first, last)] = term[
                way, s, :, first:last
            ].astype(sums.dtype)
        for way in range(2):
            remote_part(r, way, first, last).start()

    def first_strip():
        shape = (2, STRIP, STRIP)
        term[:, 0, :, :STRIP] = jnp.zeros(shape, jnp.float32)

        @pl.loop(0, PIECES)
        def _(j):
            for copy in first_copies(j):
                copy.wait()

            @pl.when(j == 0)
            def _():
                first_g_copy().start()

            @pl.when(j == 2)
            def _():
                for s in range(1, strips):
                    first_a_copy(s).start()

            part = tokens_of(j, PIECES)
            product = matmul(
                a_vmem[0, part, : 2 * STRIP], g_vmem[0, 0, part, :STRIP]
            )
            term[:, 0, :, :STRIP] += product.reshape(shape)

        pl.semaphore_wait(barrier, 2)
        send_part(0, 0, STRIP)

        for x in range(1, STREAMS):
            for j in range(HALVES):
                a_copy(x, x, j).start()
                g_copy(x, 0, j).start()

        first_g_copy().wait()
        product = matmul(a_vmem[0, :, : 2 * STRIP], g_vmem[0, 0, :, STRIP:])
        term[:, 0, :, STRIP:] = product.reshape(2, STRIP, width - STRIP)
        send_part(0, STRIP, width)

    def next_strip(r):
        x, s = r // strips, lax.rem(r, strips)

        @pl.when(x == 0)
        def _():
            first_a_copy(s).wait()

        @pl.when((x > 0) & (s == 0))
        def _():
            for j in range(HALVES):
                a_copy(x, x, j).wait()
                g_copy(x, 0, j).wait()

        strip = strip_of(s)
        product = matmul(a_vmem[x, :, strip], g_vmem[lax.rem(x, 2), 0])
        term[:, s] = product.reshape(2, STRIP, width)
        send_part(r)

        @pl.when(r == strips - 1)
        def _():
            start_g(2)

    def communicate(h):
        n, k, _ = place(h)

        for way in range(2):
            remote(h - STREAMS, way).wait()

        @pl.when(k == 0)
        def _():
            for way in range(2):
                sums[n, :, way, :, block(k, way)] = term[way].astype(sums.dtype)

        @pl.when((k > 0) & (k < size))
        def _():
            for way in range(2):
                cols = block(k, way)
                came = sums[n, :, way, :, cols].astype(jnp.float32)
                sums[n, :, way, :, cols] = (came + term[way]).astype(sums.dtype)

        for way in range(2):
            remote(h, way).start()

    def compute(h):
        n, k, x = place(h)
        q = n // STREAMS
        i = q * size * STREAMS + k * STREAMS + x
        slot = lax.rem(i, 2)
        term[...] = jnp.zeros_like(term)

        @pl.loop(0, HALVES)
        def _(j):
            @pl.when(k == 0)
            def _():
                a_copy(n, x, j).wait()

            g_copy(i, 0, j).wait()

            @pl.when(apart(k) == 1)
            def _():
                g_copy(i, 1, j).wait()

            @pl.when((j == 0) & (i + 1 < items))
            def _():
                start_g(i + 1)

            part = tokens_of(j, HALVES)
            lhs = a_vmem[x, part, :]
            for way in range(2):
                strip = [
                    lhs[:, (2 * s + way) * STRIP : (2 * s + way + 1) * STRIP]
                    for s in range(strips)
                ]
                product = matmul(
                    jnp.concatenate(strip, axis=1),
                    g_vmem[slot, way * apart(k), part, :],
                )
                term[way] += product.reshape(strips, STRIP, width)

        @pl.when((k == size - 1) & (q < rounds - 1))
        def _():
            for j in range(HALVES):
                a_copy(n + STREAMS, x, j).start()

    barrier = pltpu.get_barrier_semaphore()
    for neighbour in (left, right):
        pl.semaphore_signal(
            barrier, inc=1, device_id={"dp": neighbour}, device_id_type=MESH
        )
    for j in range(PIECES):
        for copy in first_copies(j):
            copy.start()
    first_strip()
    pl.loop(1, STREAMS * strips)(next_strip)

    @pl.loop(STREAMS, halfsteps + 1)
    def _(t):
        @pl.when(t > STREAMS)
        def _():
            communicate(t - 1)

        @pl.when((t < halfsteps) & (lax.rem(t, per_round) // STREAMS < size))
        def _():
            compute(t)

    for h in range(halfsteps - STREAMS, halfsteps):
        for way in range(2):
            remote(h, way).wait()


def store_kernel(sums, out, sem):
    copies = [
        pltpu.make_async_copy(sums.at[n, s], out.at[n, s], sem.at[n, s])
        for n in range(sums.shape[0])
        for s in range(sums.shape[1])
    ]
    for copy in copies:
        copy.start()
    for copy in copies:
        copy.wait()


def solution(mesh):
    size = mesh.shape["dp"]

    def step(a, g):
        a, g = a[0], g[0]
        matrices, tokens, rows = a.shape
        columns = g.shape[2]
        strips, width = rows // (2 * STRIP), columns // size
        shape = (matrices, strips, 2, STRIP, columns)
        sums = pl.pallas_call(
            functools.partial(ring_kernel, size),
            out_shape=pltpu.VMEM(shape, jnp.bfloat16),
            in_specs=[pl.BlockSpec(memory_space=pltpu.HBM)] * 2,
            out_specs=pl.BlockSpec(memory_space=pltpu.VMEM),
            scratch_shapes=[
                pltpu.VMEM((STREAMS, tokens, rows), jnp.bfloat16),
                pltpu.VMEM((2, 2, tokens, width), jnp.bfloat16),
                pltpu.VMEM((2, strips, STRIP, width), jnp.float32),
                pltpu.SemaphoreType.DMA((2, PIECES)),
                pltpu.SemaphoreType.DMA((strips,)),
                pltpu.SemaphoreType.DMA((STREAMS, HALVES)),
                pltpu.SemaphoreType.DMA((2, 2, HALVES)),
                pltpu.SemaphoreType.DMA((2 * STREAMS, 2)),
                pltpu.SemaphoreType.DMA((2 * STREAMS, 2)),
            ],
            compiler_params=pltpu.CompilerParams(
                collective_id=0,
                has_side_effects=True,
                vmem_limit_bytes=36 * 1024 * 1024,
            ),
            cost_estimate=pl.CostEstimate(
                flops=2 * matrices * tokens * rows * columns,
                bytes_accessed=2 * matrices * tokens * (rows + 2 * columns),
                transcendentals=0,
            ),
        )(a, g)
        out = pl.pallas_call(
            store_kernel,
            out_shape=jax.ShapeDtypeStruct(shape, jnp.bfloat16),
            in_specs=[pl.BlockSpec(memory_space=pltpu.VMEM)],
            out_specs=pl.BlockSpec(memory_space=pltpu.HBM),
            scratch_shapes=[pltpu.SemaphoreType.DMA((matrices, strips))],
            compiler_params=pltpu.CompilerParams(vmem_limit_bytes=20 * 1024 * 1024),
        )(sums)
        return out.reshape(matrices, rows, columns)

    return jax.shard_map(
        step,
        mesh=mesh,
        in_specs=(P(("rep", "dp")), P(("rep", "dp"))),
        out_specs=P("rep"),
        check_vma=False,
    )
```

```python
import functools

import jax
import jax.numpy as jnp
from jax import lax
from jax.experimental import pallas as pl
from jax.experimental.pallas import tpu as pltpu
from jax.sharding import PartitionSpec as P

MESH = pl.DeviceIdType.MESH
STREAMS = 2
HALVES = 2
PIECES = 4
STRIP = 128


def ring_kernel(
    size,
    a_hbm,
    g_hbm,
    sums,
    a_vmem,
    g_vmem,
    term,
    first_sem,
    strip_sem,
    a_sem,
    g_sem,
    send_sem,
    recv_sem,
):
    matrices, tokens, rows = a_hbm.shape
    columns = g_hbm.shape[2]
    strips, width = rows // (2 * STRIP), columns // size
    rounds = matrices // STREAMS
    per_round = 2 * (size - 1) * STREAMS
    halfsteps = rounds * per_round
    items = rounds * size * STREAMS
    me = lax.axis_index("dp")
    right, left = lax.rem(me + 1, size), lax.rem(me + size - 1, size)

    def place(h):
        r = lax.rem(h, per_round)
        x = lax.rem(r, STREAMS)
        return (h // per_round) * STREAMS + x, r // STREAMS, x

    def block(k, way, first=0, last=width):
        c = lax.rem(me + 2 * size + (k if way else -k), size)
        return pl.ds(pl.multiple_of(c * width + first, STRIP), last - first)

    def tokens_of(j, count):
        part = tokens // count
        return pl.ds(pl.multiple_of(j * part, part), part)

    def a_copy(n, x, j):
        part = tokens_of(j, HALVES)
        return pltpu.make_async_copy(
            a_hbm.at[n, part, :], a_vmem.at[x, part, :], a_sem.at[x, j]
        )

    def strip_of(s):
        return pl.ds(pl.multiple_of(2 * STRIP * s, 2 * STRIP), 2 * STRIP)

    def first_copies(j):
        part = tokens_of(j, PIECES)
        return (
            pltpu.make_async_copy(
                a_hbm.at[0, part, strip_of(0)],
                a_vmem.at[0, part, strip_of(0)],
                first_sem.at[0, j],
            ),
            pltpu.make_async_copy(
                g_hbm.at[0, part, block(0, 0, 0, STRIP)],
                g_vmem.at[0, 0, part, pl.ds(0, STRIP)],
                first_sem.at[1, j],
            ),
        )

    def first_g_copy():
        return pltpu.make_async_copy(
            g_hbm.at[0, :, block(0, 0, STRIP, width)],
            g_vmem.at[0, 0, :, pl.ds(STRIP, width - STRIP)],
            g_sem.at[0, 0, 0],
        )

    def first_a_copy(s):
        return pltpu.make_async_copy(
            a_hbm.at[0, :, strip_of(s)], a_vmem.at[0, :, strip_of(s)], strip_sem.at[s]
        )

    def item_place(i):
        q, r = i // (size * STREAMS), lax.rem(i, size * STREAMS)
        return q * STREAMS + lax.rem(r, STREAMS), r // STREAMS

    def g_copy(i, way, j):
        n, k = item_place(i)
        slot = lax.rem(i, 2)
        return pltpu.make_async_copy(
            g_hbm.at[n, tokens_of(j, HALVES), block(k, way)],
            g_vmem.at[slot, way, tokens_of(j, HALVES), :],
            g_sem.at[slot, way, j],
        )

    def apart(k):
        return (lax.rem(k, size // 2) + size // 2 - 1) // (size // 2)

    def start_g(i):
        _, k = item_place(i)
        for j in range(HALVES):
            g_copy(i, 0, j).start()

            @pl.when(apart(k) == 1)
            def _():
                g_copy(i, 1, j).start()

    def remote(h, way):
        n, k, _ = place(h)
        ref = sums.at[n, :, way, :, block(k, way)]
        sem = lax.rem(h, 2 * STREAMS)
        return pltpu.make_async_remote_copy(
            src_ref=ref,
            dst_ref=ref,
            send_sem=send_sem.at[sem, way],
            recv_sem=recv_sem.at[sem, way],
            device_id={"dp": left if way else right},
            device_id_type=MESH,
        )

    def remote_part(r, way, first=0, last=width):
        x, s = r // strips, lax.rem(r, strips)
        ref = sums.at[x, s, way, :, block(0, way, first, last)]
        return pltpu.make_async_remote_copy(
            src_ref=ref,
            dst_ref=ref,
            send_sem=send_sem.at[x, way],
            recv_sem=recv_sem.at[x, way],
            device_id={"dp": left if way else right},
            device_id_type=MESH,
        )

    def matmul(lhs, rhs):
        return lax.dot_general(
            lhs, rhs, (((0,), (0,)), ((), ())), preferred_element_type=jnp.float32
        )

    def send_part(r, first=0, last=width):
        x, s = r // strips, lax.rem(r, strips)
        for way in range(2):
            sums[x, s, way, :, block(0, way, first, last)] = term[
                way, s, :, first:last
            ].astype(sums.dtype)
        for way in range(2):
            remote_part(r, way, first, last).start()

    def first_strip():
        shape = (2, STRIP, STRIP)
        term[:, 0, :, :STRIP] = jnp.zeros(shape, jnp.float32)

        @pl.loop(0, PIECES)
        def _(j):
            for copy in first_copies(j):
                copy.wait()

            @pl.when(j == 0)
            def _():
                first_g_copy().start()

            @pl.when(j == 2)
            def _():
                for s in range(1, strips):
                    first_a_copy(s).start()

            part = tokens_of(j, PIECES)
            product = matmul(
                a_vmem[0, part, : 2 * STRIP], g_vmem[0, 0, part, :STRIP]
            )
            term[:, 0, :, :STRIP] += product.reshape(shape)

        pl.semaphore_wait(barrier, 2)
        send_part(0, 0, STRIP)

        for x in range(1, STREAMS):
            for j in range(HALVES):
                a_copy(x, x, j).start()
                g_copy(x, 0, j).start()

        first_g_copy().wait()
        product = matmul(a_vmem[0, :, : 2 * STRIP], g_vmem[0, 0, :, STRIP:])
        term[:, 0, :, STRIP:] = product.reshape(2, STRIP, width - STRIP)
        send_part(0, STRIP, width)

    def next_strip(r):
        x, s = r // strips, lax.rem(r, strips)

        @pl.when(x == 0)
        def _():
            first_a_copy(s).wait()

        @pl.when((x > 0) & (s == 0))
        def _():
            for j in range(HALVES):
                a_copy(x, x, j).wait()
                g_copy(x, 0, j).wait()

        strip = strip_of(s)
        product = matmul(a_vmem[x, :, strip], g_vmem[lax.rem(x, 2), 0])
        term[:, s] = product.reshape(2, STRIP, width)
        send_part(r)

        @pl.when(r == strips - 1)
        def _():
            start_g(2)

    def communicate(h):
        n, k, _ = place(h)

        for way in range(2):
            remote(h - STREAMS, way).wait()

        @pl.when(k == 0)
        def _():
            for way in range(2):
                sums[n, :, way, :, block(k, way)] = term[way].astype(sums.dtype)

        @pl.when((k > 0) & (k < size))
        def _():
            for way in range(2):
                cols = block(k, way)
                came = sums[n, :, way, :, cols].astype(jnp.float32)
                sums[n, :, way, :, cols] = (came + term[way]).astype(sums.dtype)

        for way in range(2):
            remote(h, way).start()

    def compute(h):
        n, k, x = place(h)
        q = n // STREAMS
        i = q * size * STREAMS + k * STREAMS + x
        slot = lax.rem(i, 2)
        term[...] = jnp.zeros_like(term)

        @pl.loop(0, HALVES)
        def _(j):
            @pl.when(k == 0)
            def _():
                a_copy(n, x, j).wait()

            g_copy(i, 0, j).wait()

            @pl.when(apart(k) == 1)
            def _():
                g_copy(i, 1, j).wait()

            @pl.when((j == 0) & (i + 1 < items))
            def _():
                start_g(i + 1)

            part = tokens_of(j, HALVES)
            lhs = a_vmem[x, part, :]
            for way in range(2):
                strip = [
                    lhs[:, (2 * s + way) * STRIP : (2 * s + way + 1) * STRIP]
                    for s in range(strips)
                ]
                product = matmul(
                    jnp.concatenate(strip, axis=1),
                    g_vmem[slot, way * apart(k), part, :],
                )
                term[way] += product.reshape(strips, STRIP, width)

        @pl.when((k == size - 1) & (q < rounds - 1))
        def _():
            for j in range(HALVES):
                a_copy(n + STREAMS, x, j).start()

    for j in range(PIECES):
        for copy in first_copies(j):
            copy.start()
    barrier = pltpu.get_barrier_semaphore()
    for neighbour in (left, right):
        pl.semaphore_signal(
            barrier, inc=1, device_id={"dp": neighbour}, device_id_type=MESH
        )
    first_strip()
    pl.loop(1, STREAMS * strips)(next_strip)

    @pl.loop(STREAMS, halfsteps + 1)
    def _(t):
        @pl.when(t > STREAMS)
        def _():
            communicate(t - 1)

        @pl.when((t < halfsteps) & (lax.rem(t, per_round) // STREAMS < size))
        def _():
            compute(t)

    for h in range(halfsteps - STREAMS, halfsteps):
        for way in range(2):
            remote(h, way).wait()


def store_kernel(sums, out, sem):
    copies = [
        pltpu.make_async_copy(sums.at[n, s], out.at[n, s], sem.at[n, s])
        for n in range(sums.shape[0])
        for s in range(sums.shape[1])
    ]
    for copy in copies:
        copy.start()
    for copy in copies:
        copy.wait()


def solution(mesh):
    size = mesh.shape["dp"]

    def step(a, g):
        a, g = a[0], g[0]
        matrices, tokens, rows = a.shape
        columns = g.shape[2]
        strips, width = rows // (2 * STRIP), columns // size
        shape = (matrices, strips, 2, STRIP, columns)
        sums = pl.pallas_call(
            functools.partial(ring_kernel, size),
            out_shape=pltpu.VMEM(shape, jnp.bfloat16),
            in_specs=[pl.BlockSpec(memory_space=pltpu.HBM)] * 2,
            out_specs=pl.BlockSpec(memory_space=pltpu.VMEM),
            scratch_shapes=[
                pltpu.VMEM((STREAMS, tokens, rows), jnp.bfloat16),
                pltpu.VMEM((2, 2, tokens, width), jnp.bfloat16),
                pltpu.VMEM((2, strips, STRIP, width), jnp.float32),
                pltpu.SemaphoreType.DMA((2, PIECES)),
                pltpu.SemaphoreType.DMA((strips,)),
                pltpu.SemaphoreType.DMA((STREAMS, HALVES)),
                pltpu.SemaphoreType.DMA((2, 2, HALVES)),
                pltpu.SemaphoreType.DMA((2 * STREAMS, 2)),
                pltpu.SemaphoreType.DMA((2 * STREAMS, 2)),
            ],
            compiler_params=pltpu.CompilerParams(
                collective_id=0,
                has_side_effects=True,
                vmem_limit_bytes=36 * 1024 * 1024,
            ),
            cost_estimate=pl.CostEstimate(
                flops=2 * matrices * tokens * rows * columns,
                bytes_accessed=2 * matrices * tokens * (rows + 2 * columns),
                transcendentals=0,
            ),
        )(a, g)
        out = pl.pallas_call(
            store_kernel,
            out_shape=jax.ShapeDtypeStruct(shape, jnp.bfloat16),
            in_specs=[pl.BlockSpec(memory_space=pltpu.VMEM)],
            out_specs=pl.BlockSpec(memory_space=pltpu.HBM),
            scratch_shapes=[pltpu.SemaphoreType.DMA((matrices, strips))],
            compiler_params=pltpu.CompilerParams(vmem_limit_bytes=20 * 1024 * 1024),
        )(sums)
        return out.reshape(matrices, rows, columns)

    return jax.shard_map(
        step,
        mesh=mesh,
        in_specs=(P(("rep", "dp")), P(("rep", "dp"))),
        out_specs=P("rep"),
        check_vma=False,
    )
```
